32 devices in a mesh: row: 8 (over z, x), col: 4 (over y, core).
Axes of the slice: x: 2, y: 2, z: 4, core: 2. Of those that a mesh axis runs over, the one named last changes fastest.
Arguments:
- frontier: bfloat16 [8192, 128], P(('row', 'col')), may hold values from 0 to 8, as said below
- visited: int32 [8192, 128], P(('row', 'col')), may hold values 0 or 1
- tile_rows: int32 [8, 4, 8, 20], P('row', 'col'), may hold values from 0 to 1
- tile_cols: int32 [8, 4, 8, 20], P('row', 'col'), may hold values from 0 to 7
- tile_bits: bfloat16 [8, 4, 8, 20, 128, 128], P('row', 'col'), may hold values from 0 to 1, as said below
Outputs:
- depth_out: int32 [8192, 128], P(('row', 'col'))
- reach_out: float32 [8192, 128], P(('row', 'col'))
The draws below stay inside these ranges and needn't reach their ends.
Inputs may be any that keep to these rules, and one draw needn't show every extreme that they name: `frontier`: every entry is 0 or lies between 0.25 and 8. `tile_bits`: entries are 0 or 1.
All inputs are finite; a program needn't handle non-finite values. No bound on the sum of `visited` on one device may be relied on, other than what follows from the above.
Results may differ from the reference program's by a relative error of at most 0.0065.
Values may be sent and summed in bfloat16 or wider, within the bound.
A program may use at most 64 MiB of HBM per device.

```python
import jax
import jax.numpy as jnp
from jax import lax

SOURCES = 128
TILE = 128
VERT_DEV = 256
TILES_DEV = 160
LEVELS = 4
VERTICES = 8192
SLOTS = 20
N_ROW = 8
N_COL = 4


def draw_frontier(key, part):
    key_live = jax.random.fold_in(key, 11)
    key_value = jax.random.fold_in(key, 12)
    key_order = jax.random.fold_in(key, 13)
    key_rate = jax.random.fold_in(key, 14)
    blocks = N_ROW * N_COL
    shape = (VERT_DEV * blocks, SOURCES)
    order = jax.random.permutation(key_order, SOURCES)
    dead_count = max(SOURCES // 16, 1)
    weak_count = max(SOURCES // 4, 1)
    dense_count = max(SOURCES // 4, 1)
    dead = order < dead_count
    weak = (order >= dead_count) & (order < dead_count + weak_count)
    dense = (order >= dead_count + weak_count) & (order < dead_count + weak_count + dense_count)
    rate_spread = jax.random.uniform(key_rate, (blocks, SOURCES), jnp.float32)
    block_rates = jnp.exp(jnp.log(0.03) + (jnp.log(0.5) - jnp.log(0.03)) * rate_spread)
    vertex_rates = jnp.repeat(block_rates, VERT_DEV, axis=0)
    rates = jnp.where(dense[None, :], vertex_rates, 0.003)
    live = (jax.random.uniform(key_live, shape, jnp.float32) < rates) & jnp.logical_not(dead)[None, :]
    spread = jax.random.uniform(key_value, shape, jnp.float32)
    strong_values = jnp.exp(jnp.log(0.5) + (jnp.log(4.0) - jnp.log(0.5)) * spread)
    weak_values = jnp.exp(jnp.log(0.25) + (jnp.log(0.8) - jnp.log(0.25)) * spread)
    values = jnp.where(weak[None, :], weak_values, strong_values)
    return jnp.where(live, values, 0.0).astype(jnp.float32).astype(jnp.bfloat16)


def draw_tile_bits(key, part):
    density = 16.0 * VERT_DEV / (TILES_DEV * TILE * TILE)
    shape = (N_ROW, N_COL, N_ROW, SLOTS, TILE, TILE)
    edges = jax.random.uniform(jax.random.fold_in(key, 21), shape, jnp.float32) < density
    return edges.astype(jnp.float32).astype(jnp.bfloat16)


def place_ends(entries, stream_key, smallest, top_value):
    place = [jax.random.randint(jax.random.fold_in(stream_key, axis), (), 0, length) for axis, length in enumerate(entries.shape)]
    main_axis = entries.shape.index(max(entries.shape))
    neighbour = place[:main_axis] + [(place[main_axis] + 1) % entries.shape[main_axis]] + place[main_axis + 1:]
    return entries.at[tuple(place)].set(smallest).at[tuple(neighbour)].set(top_value)


def setup_inputs(seed: int = 0) -> dict:
    splits = jax.random.split(jax.random.key(seed), 6)
    frontier = draw_frontier(jax.random.fold_in(splits[5], 71), 0)
    visited = place_ends((jax.random.randint(splits[1], (VERTICES, SOURCES), 0, 4) < 1).astype(jnp.int32), jax.random.fold_in(splits[1], 1), 0, 1)
    tile_rows = place_ends(jax.random.randint(splits[2], (N_ROW, N_COL, N_ROW, SLOTS), 0, VERT_DEV // TILE), jax.random.fold_in(splits[2], 1), 0, (VERT_DEV // TILE) - 1).astype(jnp.int32)
    tile_cols = place_ends(jax.random.randint(splits[3], (N_ROW, N_COL, N_ROW, SLOTS), 0, N_COL * VERT_DEV // TILE), jax.random.fold_in(splits[3], 1), 0, (N_COL * VERT_DEV // TILE) - 1).astype(jnp.int32)
    tile_bits = draw_tile_bits(jax.random.fold_in(splits[5], 71), 0)
    return dict(frontier=frontier, visited=visited, tile_rows=tile_rows, tile_cols=tile_cols, tile_bits=tile_bits)


def expand(current, tile_rows, tile_cols, tile_bits):
    width = current.shape[1]
    col_tiles = N_COL * VERT_DEV // TILE
    blocked = current.reshape(N_ROW, N_COL, VERT_DEV // TILE, TILE, width)

    def one_row(row_pos):
        def one_device(running, col_pos):
            source_part = lax.dynamic_index_in_dim(blocked, col_pos, 1, keepdims=False)
            row_ids = tile_rows[row_pos, col_pos]
            col_ids = tile_cols[row_pos, col_pos]
            edge_bits = tile_bits[row_pos, col_pos].astype(jnp.float32)
            picked = jnp.take_along_axis(source_part, row_ids[:, :, None, None], axis=1).astype(jnp.float32)
            products = jnp.einsum("qtkn,qtks->qtns", edge_bits, picked, precision=lax.Precision.HIGHEST)
            summed = jax.ops.segment_sum(products.reshape(-1, TILE, width), col_ids.reshape(-1).astype(jnp.int32), num_segments=col_tiles)
            rounded = lax.optimization_barrier(summed.astype(jnp.bfloat16))
            return running + rounded.astype(jnp.float32), None

        zero_sums = jnp.zeros((col_tiles, TILE, width), jnp.float32)
        running, unused = lax.scan(one_device, zero_sums, jnp.arange(N_COL, dtype=jnp.int32))
        return running

    result = lax.map(one_row, jnp.arange(N_ROW, dtype=jnp.int32))
    return result.reshape(-1, width)


def reference(frontier, visited, tile_rows, tile_cols, tile_bits):
    visited_now = (visited != 0) | (frontier > 0)
    depth_out = jnp.where(visited_now, 0, LEVELS + 1).astype(jnp.int32)
    reach_out = frontier.astype(jnp.float32)
    scaling = jnp.ones((SOURCES,), jnp.float32)
    current = frontier
    for level_step in range(1, LEVELS + 1):
        raw_sum = expand(current, tile_rows, tile_cols, tile_bits)
        newly_hit = (raw_sum > 0) & jnp.logical_not(visited_now)
        reached = jnp.where(newly_hit, raw_sum, jnp.zeros_like(raw_sum))
        counted = jnp.sum(newly_hit.astype(jnp.float32), axis=0)
        totals = jnp.sum(reached, axis=0)
        scaling = scaling / jnp.maximum(scaling * totals / jnp.maximum(counted, 1.0), 1.0)
        reach_out = reach_out + scaling[None, :] * reached
        depth_out = jnp.where(newly_hit, level_step, depth_out).astype(jnp.int32)
        visited_now = visited_now | newly_hit
        current = reached.astype(jnp.bfloat16)
    return depth_out, reach_out
```

```python
import functools

import jax
import jax.numpy as jnp
from jax import lax
from jax.experimental import pallas as pl
from jax.experimental.pallas import tpu as pltpu
from jax.sharding import PartitionSpec as P

LEVELS = 4
HALVES = 1
MESH = pl.DeviceIdType.MESH


def dense_kernel(rows_ref, cols_ref, tiles_ref, out_ref):
    q = pl.program_id(0)
    slots, tile = tiles_ref.shape[1], tiles_ref.shape[-1]
    per_chunk = out_ref.shape[-1] // tile
    out_ref[...] = jnp.zeros_like(out_ref)

    def add(s, carry):
        r = rows_ref[q, s]
        c = cols_ref[q, s]
        at = (
            0,
            c // per_chunk,
            pl.ds(pl.multiple_of(r * tile, tile), tile),
            pl.ds(pl.multiple_of((c % per_chunk) * tile, tile), tile),
        )
        out_ref[at] = out_ref[at] + tiles_ref[0, s]
        return carry

    lax.fori_loop(0, slots, add, 0, unroll=2)


def densify(rows, cols, tiles, n_col, per_dev):
    blocks, slots, tile, unused = tiles.shape
    return pl.pallas_call(
        dense_kernel,
        grid=(blocks,),
        out_shape=jax.ShapeDtypeStruct((blocks, n_col, per_dev, per_dev), jnp.bfloat16),
        in_specs=[
            pl.BlockSpec(memory_space=pltpu.SMEM),
            pl.BlockSpec(memory_space=pltpu.SMEM),
            pl.BlockSpec((1, slots, tile, tile), lambda q: (q, 0, 0, 0)),
        ],
        out_specs=pl.BlockSpec((1, n_col, per_dev, per_dev), lambda q: (q, 0, 0, 0)),
        name="densify",
    )(rows, cols, tiles)


def search_kernel(
    n_row, n_col, n_x, n_core,
    frontier_ref, visited_ref, adj_hbm, depth_out, reach_out,
    adj, cur, acc, part, got, depth_t, held_t, stat_c, stat_r,
    load_sem, ag_send, ag_recv, rs_send, rs_recv, sc_send, sc_recv, sr_send, sr_recv,
):
    n_z = n_row // n_x
    n_y = n_col // n_core
    row, col = lax.axis_index("row"), lax.axis_index("col")
    z, x = row // n_x, row % n_x
    y, core = col // n_core, col % n_core
    halves, width = cur.shape[1], cur.shape[3]

    z_steps = []
    for d in range(1, n_z // 2 + 1):
        z_steps += [d] if d == n_z - d else [d, n_z - d]
    z_peers = [((z + d) % n_z) * n_x + x for d in z_steps]
    x_peers = [z * n_x + (x + d) % n_x for d in range(1, n_x)]
    far_peers = [
        ((z + d) % n_z) * n_x + (x + e) % n_x for d in z_steps for e in range(1, n_x)
    ]
    c_peers = [
        ((y + d) % n_y) * n_core + (core + e) % n_core
        for d in range(1, n_y) for e in range(n_core)
    ] + [y * n_core + (core + e) % n_core for e in range(1, n_core)]
    r_peers = x_peers + z_peers + far_peers

    barrier = pltpu.get_barrier_semaphore()
    for p in r_peers:
        pl.semaphore_signal(barrier, inc=1, device_id=(p, col), device_id_type=MESH)
    for p in c_peers:
        pl.semaphore_signal(barrier, inc=1, device_id=(row, p), device_id_type=MESH)

    loads = [pltpu.make_async_copy(adj_hbm.at[q], adj.at[q], load_sem.at[q]) for q in range(n_row)]
    for load in loads:
        load.start()

    start = frontier_ref[...].astype(jnp.float32).T
    for h in range(halves):
        cur[0, h, row] = start[h * width:(h + 1) * width].astype(jnp.bfloat16)
    seen = (visited_ref[...].T != 0) | (start > 0)
    depth_t[...] = jnp.where(seen, 0, LEVELS + 1)
    held_t[...] = jnp.zeros_like(held_t)

    pl.semaphore_wait(barrier, len(r_peers) + len(c_peers))

    def gather_copy(level, h, q, k, peer):
        par = level % 2
        block = cur.at[level, h, q]
        return pltpu.make_async_remote_copy(
            src_ref=block, dst_ref=block,
            send_sem=ag_send.at[par, h, k], recv_sem=ag_recv.at[par, h, q],
            device_id=(peer, col), device_id_type=MESH,
        )

    def scatter_copy(level, h, d, src_col, peer):
        par = level % 2
        return pltpu.make_async_remote_copy(
            src_ref=part.at[level, h, d], dst_ref=got.at[level, h, src_col],
            send_sem=rs_send.at[par, h, d], recv_sem=rs_recv.at[par, h, src_col],
            device_id=(row, peer), device_id_type=MESH,
        )

    def send_own(level, h):
        for k, p in enumerate(x_peers + z_peers):
            gather_copy(level, h, row, k, p).start()

    for h in range(halves):
        send_own(0, h)
    for load in loads:
        load.wait()

    def multiply(level, h, q, first):
        block = cur[level, h, q]
        for c in range(n_col):
            prod = jnp.dot(block, adj[q, c], preferred_element_type=jnp.float32)
            acc[c] = prod if first else acc[c] + prod

    def one_level(level, carry):
        for h in range(halves):
            k = len(x_peers) + len(z_peers)
            multiply(level, h, row, True)
            for q in z_peers:
                gather_copy(level, h, q, 0, q).wait_recv()
                for p in x_peers:
                    gather_copy(level, h, q, k, p).start()
                    k += 1
                multiply(level, h, q, False)
            tail = x_peers + far_peers
            for q in tail[:-1]:
                gather_copy(level, h, q, 0, q).wait_recv()
                multiply(level, h, q, False)
            last = tail[-1]
            gather_copy(level, h, last, 0, last).wait_recv()
            block = cur[level, h, last]
            for d, p in enumerate(c_peers + [col]):
                total = acc[p] + jnp.dot(block, adj[last, p], preferred_element_type=jnp.float32)
                part[level, h, d] = total.astype(jnp.bfloat16)
                if d < len(c_peers):
                    scatter_copy(level, h, d, col, p).start()
        for h in range(halves):
            here = slice(h * width, (h + 1) * width)
            raw = part[level, h, len(c_peers)].astype(jnp.float32)
            for p in reversed(c_peers):
                scatter_copy(level, h, 0, p, p).wait_recv()
                raw = raw + got[level, h, p].astype(jnp.float32)
            depth = depth_t[here, :]
            fresh = (raw > 0) & (depth == LEVELS + 1)
            held = jnp.where(fresh, raw, 0.0)
            cur[level + 1, h, row] = held.astype(jnp.bfloat16)

            depth_t[here, :] = jnp.where(fresh, level + 1, depth)
            held_t[here, :] = held_t[here, :] + held

            @pl.when(level < LEVELS - 1)
            def _():
                send_own(level + 1, h)
        for h in range(halves):
            for k, p in enumerate(r_peers):
                gather_copy(level, h, row, k, p).wait_send()
            for d, p in enumerate(c_peers):
                scatter_copy(level, h, d, col, p).wait_send()
        return carry

    lax.fori_loop(0, LEVELS, one_level, 0)

    depth = depth_t[...].T
    held = held_t[...].T
    rows = []
    for level in range(1, LEVELS + 1):
        hit = depth == level
        rows.append(jnp.sum(hit.astype(jnp.float32), axis=0, keepdims=True))
        rows.append(jnp.sum(jnp.where(hit, held, 0.0), axis=0, keepdims=True))
    stat_c[col] = jnp.concatenate(rows, axis=0)
    depth_out[...] = depth

    def stat_copy(buf, mine, k, send, recv, device):
        return pltpu.make_async_remote_copy(
            src_ref=buf.at[mine], dst_ref=buf.at[mine],
            send_sem=send.at[k], recv_sem=recv.at[mine],
            device_id=device, device_id_type=MESH,
        )

    def spread(buf, me, peers, send, recv, device):
        for k, p in enumerate(peers):
            stat_copy(buf, me, k, send, recv, device(p)).start()
        total = buf[me]
        for p in peers:
            stat_copy(buf, p, 0, send, recv, device(p)).wait_recv()
            total = total + buf[p]
        for k, p in enumerate(peers):
            stat_copy(buf, me, k, send, recv, device(p)).wait_send()
        return total

    stat_r[row] = spread(stat_c, col, c_peers, sc_send, sc_recv, lambda p: (row, p))
    sums = spread(stat_r, row, r_peers, sr_send, sr_recv, lambda p: (p, col))

    scaling = jnp.ones((1, sums.shape[1]), jnp.float32)
    factor = jnp.zeros_like(held)
    for level in range(1, LEVELS + 1):
        count = sums[2 * level - 2:2 * level - 1]
        total = sums[2 * level - 1:2 * level]
        scaling = scaling / jnp.maximum(scaling * total / jnp.maximum(count, 1.0), 1.0)
        factor = jnp.where(depth == level, scaling, factor)
    reach_out[...] = frontier_ref[...].astype(jnp.float32) + factor * held


def search(frontier, visited, adj, n_row, n_col):
    per_dev, sources = frontier.shape
    n_core = 2 if n_col % 2 == 0 else 1
    n_x = n_col // n_core
    n_x = n_x if n_row % n_x == 0 else 1
    width = sources // HALVES
    dma = pltpu.SemaphoreType.DMA
    vmem = pl.BlockSpec(memory_space=pltpu.VMEM)
    return pl.pallas_call(
        functools.partial(search_kernel, n_row, n_col, n_x, n_core),
        out_shape=(
            jax.ShapeDtypeStruct((per_dev, sources), jnp.int32),
            jax.ShapeDtypeStruct((per_dev, sources), jnp.float32),
        ),
        in_specs=[vmem, vmem, pl.BlockSpec(memory_space=pl.ANY)],
        out_specs=(vmem, vmem),
        scratch_shapes=[
            pltpu.VMEM((n_row, n_col, per_dev, per_dev), jnp.bfloat16),
            pltpu.VMEM((LEVELS + 1, HALVES, n_row, width, per_dev), jnp.bfloat16),
            pltpu.VMEM((n_col, width, per_dev), jnp.float32),
            pltpu.VMEM((LEVELS, HALVES, n_col, width, per_dev), jnp.bfloat16),
            pltpu.VMEM((LEVELS, HALVES, n_col, width, per_dev), jnp.bfloat16),
            pltpu.VMEM((sources, per_dev), jnp.int32),
            pltpu.VMEM((sources, per_dev), jnp.float32),
            pltpu.VMEM((n_col, 2 * LEVELS, sources), jnp.float32),
            pltpu.VMEM((n_row, 2 * LEVELS, sources), jnp.float32),
            dma((n_row,)),
            dma((2, HALVES, n_row)),
            dma((2, HALVES, n_row)),
            dma((2, HALVES, n_col)),
            dma((2, HALVES, n_col)),
            dma((n_col,)),
            dma((n_col,)),
            dma((n_row,)),
            dma((n_row,)),
        ],
        compiler_params=pltpu.CompilerParams(
            collective_id=0, has_side_effects=True, vmem_limit_bytes=60 * 1024 * 1024
        ),
        name="search",
    )(frontier, visited, adj)


def solution(mesh):
    n_row, n_col = mesh.shape["row"], mesh.shape["col"]

    def on_device(frontier, visited, tile_rows, tile_cols, tile_bits):
        per_dev = frontier.shape[0]
        adj = densify(tile_rows[0, 0], tile_cols[0, 0], tile_bits[0, 0], n_col, per_dev)
        return search(frontier, visited, adj, n_row, n_col)

    placed = (
        P(("row", "col"), None),
        P(("row", "col"), None),
        P("row", "col", None, None),
        P("row", "col", None, None),
        P("row", "col", None, None, None, None),
    )
    return jax.shard_map(
        on_device,
        mesh=mesh,
        in_specs=placed,
        out_specs=(P(("row", "col"), None), P(("row", "col"), None)),
        check_vma=False,
    )
```

```python
import functools

import jax
import jax.numpy as jnp
from jax import lax
from jax.experimental import pallas as pl
from jax.experimental.pallas import tpu as pltpu
from jax.sharding import PartitionSpec as P

LEVELS = 4
HALVES = 2
MESH = pl.DeviceIdType.MESH


def search_kernel(
    n_row, n_col, n_x, n_core,
    frontier_ref, visited_ref, rows_ref, cols_ref, tiles_hbm, depth_out, reach_out,
    tiles, key_v, prev_v, last_v, prev_s, last_s, adj, cur, acc, part, got, depth_t, held_t, stat_c, stat_r,
    load_sem, index_sem, ag_send, ag_recv, rs_send, rs_recv, sc_send, sc_recv, sr_send, sr_recv,
):
    n_z = n_row // n_x
    n_y = n_col // n_core
    row, col = lax.axis_index("row"), lax.axis_index("col")
    z, x = row // n_x, row % n_x
    y, core = col // n_core, col % n_core
    halves, width = cur.shape[1], cur.shape[3]

    z_steps = []
    for d in range(1, n_z // 2 + 1):
        z_steps += [d] if d == n_z - d else [d, n_z - d]
    z_peers = [((z + d) % n_z) * n_x + x for d in z_steps]
    x_peers = [z * n_x + (x + d) % n_x for d in range(1, n_x)]
    far_peers = [
        ((z + d) % n_z) * n_x + (x + e) % n_x for d in z_steps for e in range(1, n_x)
    ]
    c_peers = [
        ((y + d) % n_y) * n_core + (core + e) % n_core
        for d in range(1, n_y) for e in range(n_core)
    ] + [y * n_core + (core + e) % n_core for e in range(1, n_core)]
    r_peers = x_peers + z_peers + far_peers

    barrier = pltpu.get_barrier_semaphore()
    for p in r_peers:
        pl.semaphore_signal(barrier, inc=1, device_id=(p, col), device_id_type=MESH)
    for p in c_peers:
        pl.semaphore_signal(barrier, inc=1, device_id=(row, p), device_id_type=MESH)

    slots, tile = tiles_hbm.shape[1], tiles_hbm.shape[-1]
    per_chunk = adj.shape[-1] // tile
    loads = [
        pltpu.make_async_copy(tiles_hbm.at[q], tiles.at[q, pl.ds(0, slots)], load_sem.at[q])
        for q in range(n_row)
    ]
    for load in loads:
        load.start()

    key_v[...] = jnp.full_like(key_v, -1)
    key_v[:, pl.ds(0, slots)] = rows_ref[...] * (n_col * per_chunk) + cols_ref[...]
    key = key_v[...]
    lane = lax.broadcasted_iota(jnp.int32, key.shape, 1)
    prev = jnp.full(key.shape, slots, jnp.int32)
    last = jnp.full(key.shape, slots, jnp.int32)
    for t in range(slots):
        this = key[:, t:t + 1]
        prev = jnp.where((this == key) & (lane > t), t, prev)
        last = jnp.where(this == lane, t, last)
    prev_v[...] = prev
    last_v[...] = last
    tables = [
        pltpu.make_async_copy(prev_v, prev_s, index_sem.at[0]),
        pltpu.make_async_copy(last_v, last_s, index_sem.at[1]),
    ]
    for table in tables:
        table.start()
    for q in range(n_row):
        tiles[q, slots] = jnp.zeros((tile, tile), jnp.bfloat16)

    start = frontier_ref[...].astype(jnp.float32).T
    for h in range(halves):
        cur[0, h, row] = start[h * width:(h + 1) * width].astype(jnp.bfloat16)
    seen = (visited_ref[...].T != 0) | (start > 0)
    depth_t[...] = jnp.where(seen, 0, LEVELS + 1)
    held_t[...] = jnp.zeros_like(held_t)

    for table in tables:
        table.wait()
    for load in loads:
        load.wait()

    def chain(s, carry):
        for q in range(0, n_row, 4):
            group = range(q, min(q + 4, n_row))
            sums = [tiles[g, s] + tiles[g, prev_s[g, s]] for g in group]
            for g, total in zip(group, sums):
                tiles[g, s] = total
        return carry

    lax.fori_loop(1, slots, chain, 0)

    def place(q, carry):
        for r in range(adj.shape[2] // tile):
            for c in range(n_col * per_chunk):
                low = (c % per_chunk) * tile
                adj[q, c // per_chunk, r * tile:(r + 1) * tile, low:low + tile] = (
                    tiles[q, last_s[q, r * n_col * per_chunk + c]]
                )
        return carry

    pl.semaphore_wait(barrier, len(r_peers) + len(c_peers))

    def gather_copy(level, h, q, k, peer):
        par = level % 2
        block = cur.at[level, h, q]
        return pltpu.make_async_remote_copy(
            src_ref=block, dst_ref=block,
            send_sem=ag_send.at[par, h, k], recv_sem=ag_recv.at[par, h, q],
            device_id=(peer, col), device_id_type=MESH,
        )

    def scatter_copy(level, h, d, src_col, peer):
        par = level % 2
        return pltpu.make_async_remote_copy(
            src_ref=part.at[level, h, d], dst_ref=got.at[level, h, src_col],
            send_sem=rs_send.at[par, h, d], recv_sem=rs_recv.at[par, h, src_col],
            device_id=(row, peer), device_id_type=MESH,
        )

    def send_own(level, h):
        for k, p in enumerate(x_peers + z_peers):
            gather_copy(level, h, row, k, p).start()

    for h in range(halves):
        send_own(0, h)
    lax.fori_loop(0, n_row, place, 0)

    def multiply(level, h, q, first):
        block = cur[level, h, q]
        for c in range(n_col):
            prod = jnp.dot(block, adj[q, c], preferred_element_type=jnp.float32)
            acc[h, c] = prod if first else acc[h, c] + prod

    def take_z(level, h):
        k = len(x_peers) + len(z_peers)
        multiply(level, h, row, True)
        for q in z_peers:
            gather_copy(level, h, q, 0, q).wait_recv()
            for p in x_peers:
                gather_copy(level, h, q, k, p).start()
                k += 1
            multiply(level, h, q, False)

    def take_x(level, h):
        tail = x_peers + far_peers
        for q in tail[:-1]:
            gather_copy(level, h, q, 0, q).wait_recv()
            multiply(level, h, q, False)
        last = tail[-1]
        gather_copy(level, h, last, 0, last).wait_recv()
        block = cur[level, h, last]
        for d, p in enumerate(c_peers + [col]):
            total = acc[h, p] + jnp.dot(block, adj[last, p], preferred_element_type=jnp.float32)
            part[level, h, d] = total.astype(jnp.bfloat16)
            if d < len(c_peers):
                scatter_copy(level, h, d, col, p).start()

    def close(level, h):
        here = slice(h * width, (h + 1) * width)
        raw = part[level, h, len(c_peers)].astype(jnp.float32)
        for p in reversed(c_peers):
            scatter_copy(level, h, 0, p, p).wait_recv()
            raw = raw + got[level, h, p].astype(jnp.float32)
        depth = depth_t[here, :]
        fresh = (raw > 0) & (depth == LEVELS + 1)
        held = jnp.where(fresh, raw, 0.0)
        cur[level + 1, h, row] = held.astype(jnp.bfloat16)
        depth_t[here, :] = jnp.where(fresh, level + 1, depth)
        held_t[here, :] = held_t[here, :] + held

        @pl.when(level < LEVELS - 1)
        def _():
            send_own(level + 1, h)

        for k, p in enumerate(r_peers):
            gather_copy(level, h, row, k, p).wait_send()
        for d, p in enumerate(c_peers):
            scatter_copy(level, h, d, col, p).wait_send()

    def one_level(level, carry):
        for h in range(halves - 1):
            take_x(level, h)
        take_z(level, halves - 1)
        for h in range(halves - 1):
            close(level, h)
        take_x(level, halves - 1)

        @pl.when(level < LEVELS - 1)
        def _():
            for h in range(halves - 1):
                take_z(level + 1, h)

        close(level, halves - 1)
        return carry

    for h in range(halves - 1):
        take_z(0, h)
    lax.fori_loop(0, LEVELS, one_level, 0)

    depth = depth_t[...].T
    held = held_t[...].T
    rows = []
    for level in range(1, LEVELS + 1):
        hit = depth == level
        rows.append(jnp.sum(hit.astype(jnp.float32), axis=0, keepdims=True))
        rows.append(jnp.sum(jnp.where(hit, held, 0.0), axis=0, keepdims=True))
    stat_c[col] = jnp.concatenate(rows, axis=0)
    depth_out[...] = depth

    def stat_copy(buf, mine, k, send, recv, device):
        return pltpu.make_async_remote_copy(
            src_ref=buf.at[mine], dst_ref=buf.at[mine],
            send_sem=send.at[k], recv_sem=recv.at[mine],
            device_id=device, device_id_type=MESH,
        )

    def spread(buf, me, peers, send, recv, device):
        for k, p in enumerate(peers):
            stat_copy(buf, me, k, send, recv, device(p)).start()
        total = buf[me]
        for p in peers:
            stat_copy(buf, p, 0, send, recv, device(p)).wait_recv()
            total = total + buf[p]
        for k, p in enumerate(peers):
            stat_copy(buf, me, k, send, recv, device(p)).wait_send()
        return total

    stat_r[row] = spread(stat_c, col, c_peers, sc_send, sc_recv, lambda p: (row, p))
    sums = spread(stat_r, row, r_peers, sr_send, sr_recv, lambda p: (p, col))

    scaling = jnp.ones((1, sums.shape[1]), jnp.float32)
    factor = jnp.zeros_like(held)
    for level in range(1, LEVELS + 1):
        count = sums[2 * level - 2:2 * level - 1]
        total = sums[2 * level - 1:2 * level]
        scaling = scaling / jnp.maximum(scaling * total / jnp.maximum(count, 1.0), 1.0)
        factor = jnp.where(depth == level, scaling, factor)
    reach_out[...] = frontier_ref[...].astype(jnp.float32) + factor * held


def search(frontier, visited, rows, cols, tiles, n_row, n_col):
    blocks, slots, tile, unused = tiles.shape
    per_dev, sources = frontier.shape
    places = (per_dev // tile) * (n_col * per_dev // tile)
    table = (blocks, 128 * (max(slots, places) // 128 + 1))
    n_core = 2 if n_col % 2 == 0 else 1
    n_x = n_col // n_core
    n_x = n_x if n_row % n_x == 0 else 1
    width = sources // HALVES
    dma = pltpu.SemaphoreType.DMA
    vmem = pl.BlockSpec(memory_space=pltpu.VMEM)
    return pl.pallas_call(
        functools.partial(search_kernel, n_row, n_col, n_x, n_core),
        out_shape=(
            jax.ShapeDtypeStruct((per_dev, sources), jnp.int32),
            jax.ShapeDtypeStruct((per_dev, sources), jnp.float32),
        ),
        in_specs=[vmem, vmem, vmem, vmem, pl.BlockSpec(memory_space=pl.ANY)],
        out_specs=(vmem, vmem),
        scratch_shapes=[
            pltpu.VMEM((blocks, slots + 1, tile, tile), jnp.bfloat16),
            pltpu.VMEM(table, jnp.int32),
            pltpu.VMEM(table, jnp.int32),
            pltpu.VMEM(table, jnp.int32),
            pltpu.SMEM(table, jnp.int32),
            pltpu.SMEM(table, jnp.int32),
            pltpu.VMEM((n_row, n_col, per_dev, per_dev), jnp.bfloat16),
            pltpu.VMEM((LEVELS + 1, HALVES, n_row, width, per_dev), jnp.bfloat16),
            pltpu.VMEM((HALVES, n_col, width, per_dev), jnp.float32),
            pltpu.VMEM((LEVELS, HALVES, n_col, width, per_dev), jnp.bfloat16),
            pltpu.VMEM((LEVELS, HALVES, n_col, width, per_dev), jnp.bfloat16),
            pltpu.VMEM((sources, per_dev), jnp.int32),
            pltpu.VMEM((sources, per_dev), jnp.float32),
            pltpu.VMEM((n_col, 2 * LEVELS, sources), jnp.float32),
            pltpu.VMEM((n_row, 2 * LEVELS, sources), jnp.float32),
            dma((n_row,)),
            dma((2,)),
            dma((2, HALVES, n_row)),
            dma((2, HALVES, n_row)),
            dma((2, HALVES, n_col)),
            dma((2, HALVES, n_col)),
            dma((n_col,)),
            dma((n_col,)),
            dma((n_row,)),
            dma((n_row,)),
        ],
        compiler_params=pltpu.CompilerParams(
            collective_id=0, has_side_effects=True, vmem_limit_bytes=60 * 1024 * 1024
        ),
        name="search",
    )(frontier, visited, rows, cols, tiles)


def solution(mesh):
    n_row, n_col = mesh.shape["row"], mesh.shape["col"]

    def on_device(frontier, visited, tile_rows, tile_cols, tile_bits):
        return search(
            frontier, visited, tile_rows[0, 0], tile_cols[0, 0], tile_bits[0, 0], n_row, n_col
        )

    placed = (
        P(("row", "col"), None),
        P(("row", "col"), None),
        P("row", "col", None, None),
        P("row", "col", None, None),
        P("row", "col", None, None, None, None),
    )
    return jax.shard_map(
        on_device,
        mesh=mesh,
        in_specs=placed,
        out_specs=(P(("row", "col"), None), P(("row", "col"), None)),
        check_vma=False,
    )
```

```python
import functools

import jax
import jax.numpy as jnp
from jax import lax
from jax.experimental import pallas as pl
from jax.experimental.pallas import tpu as pltpu
from jax.sharding import PartitionSpec as P

LEVELS = 4
HALVES = 2
MESH = pl.DeviceIdType.MESH


def search_kernel(
    n_row, n_col, n_x, n_core,
    frontier_ref, visited_ref, rows_ref, cols_ref, tiles_hbm, depth_out, reach_out,
    tiles, key_v, prev_v, last_v, prev_s, last_s, adj, cur, acc, part, got, depth_t, held_t, stat_c, stat_r,
    load_sem, index_sem, ag_send, ag_recv, rs_send, rs_recv, sc_send, sc_recv, sr_send, sr_recv,
    stat_f, sf_sem,
):
    n_z = n_row // n_x
    n_y = n_col // n_core
    row, col = lax.axis_index("row"), lax.axis_index("col")
    z, x = row // n_x, row % n_x
    y, core = col // n_core, col % n_core
    halves, width = cur.shape[1], cur.shape[3]

    side = z // max(n_z // 2, 1) if n_z % 2 == 0 else 0
    near = z + side * (n_z - 1 - 2 * z)
    z_rows = []
    for k in range(n_z - 1):
        t = n_z - 1 - k
        t = t - (near - t + n_z) // n_z
        z_rows.append(t + side * (n_z - 1 - 2 * t))
    z_peers = [t * n_x + x for t in z_rows]
    x_peers = [z * n_x + (x + d) % n_x for d in range(1, n_x)]
    far_peers = [
        t * n_x + (x + e) % n_x for t in reversed(z_rows) for e in range(1, n_x)
    ]
    c_peers = [
        ((y + d) % n_y) * n_core + (core + e) % n_core
        for d in range(1, n_y) for e in range(n_core)
    ] + [y * n_core + (core + e) % n_core for e in range(1, n_core)]
    r_peers = x_peers + z_peers + far_peers

    n_all = n_row * n_col
    me = row * n_col + col

    def device(k):
        p = (me + k) % n_all
        return (p // n_col, p % n_col)

    barrier = pltpu.get_barrier_semaphore()

    def greet(k, carry):
        pl.semaphore_signal(barrier, inc=1, device_id=device(k), device_id_type=MESH)
        return carry

    lax.fori_loop(1, n_all, greet, 0)

    slots, tile = tiles_hbm.shape[1], tiles_hbm.shape[-1]
    per_chunk = adj.shape[-1] // tile
    loads = [
        pltpu.make_async_copy(tiles_hbm.at[q], tiles.at[q, pl.ds(0, slots)], load_sem.at[q])
        for q in range(n_row)
    ]
    for load in loads:
        load.start()

    key_v[...] = jnp.full_like(key_v, -1)
    key_v[:, pl.ds(0, slots)] = rows_ref[...] * (n_col * per_chunk) + cols_ref[...]
    key = key_v[...]
    lane = lax.broadcasted_iota(jnp.int32, key.shape, 1)
    prev = jnp.full(key.shape, slots, jnp.int32)
    last = jnp.full(key.shape, slots, jnp.int32)
    for t in range(slots):
        this = key[:, t:t + 1]
        prev = jnp.where((this == key) & (lane > t), t, prev)
        last = jnp.where(this == lane, t, last)
    prev_v[...] = prev
    last_v[...] = last
    tables = [
        pltpu.make_async_copy(prev_v, prev_s, index_sem.at[0]),
        pltpu.make_async_copy(last_v, last_s, index_sem.at[1]),
    ]
    for table in tables:
        table.start()
    for q in range(n_row):
        tiles[q, slots] = jnp.zeros((tile, tile), jnp.bfloat16)

    start = frontier_ref[...].astype(jnp.float32).T
    for h in range(halves):
        cur[0, h, row] = start[h * width:(h + 1) * width].astype(jnp.bfloat16)
    seen = (visited_ref[...].T != 0) | (start > 0)
    depth_t[...] = jnp.where(seen, 0, LEVELS + 1)
    held_t[...] = jnp.zeros_like(held_t)

    for table in tables:
        table.wait()
    for load in loads:
        load.wait()

    def chain(s, carry):
        for q in range(0, n_row, 4):
            group = range(q, min(q + 4, n_row))
            sums = [tiles[g, s] + tiles[g, prev_s[g, s]] for g in group]
            for g, total in zip(group, sums):
                tiles[g, s] = total
        return carry


    def place(q, carry):
        for r in range(adj.shape[2] // tile):
            for c in range(n_col * per_chunk):
                low = (c % per_chunk) * tile
                adj[q, c // per_chunk, r * tile:(r + 1) * tile, low:low + tile] = (
                    tiles[q, last_s[q, r * n_col * per_chunk + c]]
                )
        return carry


    def gather_copy(level, h, q, k, peer):
        par = level % 2
        block = cur.at[level, h, q]
        return pltpu.make_async_remote_copy(
            src_ref=block, dst_ref=block,
            send_sem=ag_send.at[par, h, k], recv_sem=ag_recv.at[par, h, q],
            device_id=(peer, col), device_id_type=MESH,
        )

    def scatter_copy(level, h, d, src_col, peer):
        par = level % 2
        return pltpu.make_async_remote_copy(
            src_ref=part.at[level, h, d], dst_ref=got.at[level, h, src_col],
            send_sem=rs_send.at[par, h, d], recv_sem=rs_recv.at[par, h, src_col],
            device_id=(row, peer), device_id_type=MESH,
        )

    def send_own(level, h):
        for k, p in enumerate(x_peers + z_peers):
            gather_copy(level, h, row, k, p).start()

    pl.semaphore_wait(barrier, n_all - 1)
    for h in range(halves):
        send_own(0, h)
    lax.fori_loop(1, slots, chain, 0)
    lax.fori_loop(0, n_row, place, 0)

    def multiply(level, h, q, first):
        block = cur[level, h, q]
        for c in range(n_col):
            prod = jnp.dot(block, adj[q, c], preferred_element_type=jnp.float32)
            acc[h, c] = prod if first else acc[h, c] + prod

    def take_z(level, h):
        k = len(x_peers) + len(z_peers)
        multiply(level, h, row, True)
        for q in reversed(z_peers):
            gather_copy(level, h, q, 0, q).wait_recv()
            for p in x_peers:
                gather_copy(level, h, q, k, p).start()
                k += 1
            multiply(level, h, q, False)

    def take_x(level, h):
        tail = x_peers + far_peers
        for q in tail[:-1]:
            gather_copy(level, h, q, 0, q).wait_recv()
            multiply(level, h, q, False)
        last = tail[-1]
        gather_copy(level, h, last, 0, last).wait_recv()
        block = cur[level, h, last]
        for d, p in enumerate(c_peers + [col]):
            total = acc[h, p] + jnp.dot(block, adj[last, p], preferred_element_type=jnp.float32)
            part[level, h, d] = total.astype(jnp.bfloat16)
            if d < len(c_peers):
                scatter_copy(level, h, d, col, p).start()

    def close(level, h):
        here = slice(h * width, (h + 1) * width)
        raw = part[level, h, len(c_peers)].astype(jnp.float32)
        for p in reversed(c_peers):
            scatter_copy(level, h, 0, p, p).wait_recv()
            raw = raw + got[level, h, p].astype(jnp.float32)
        depth = depth_t[here, :]
        fresh = (raw > 0) & (depth == LEVELS + 1)
        held = jnp.where(fresh, raw, 0.0)
        cur[level + 1, h, row] = held.astype(jnp.bfloat16)
        depth_t[here, :] = jnp.where(fresh, level + 1, depth)
        held_t[here, :] = held_t[here, :] + held

        @pl.when(level < LEVELS - 1)
        def _():
            send_own(level + 1, h)

        for k, p in enumerate(r_peers):
            gather_copy(level, h, row, k, p).wait_send()
        for d, p in enumerate(c_peers):
            scatter_copy(level, h, d, col, p).wait_send()

    def stat_rows(depth, held, levels):
        rows = []
        for level in levels:
            hit = depth == level
            rows.append(jnp.sum(hit.astype(jnp.float32), axis=0, keepdims=True))
            rows.append(jnp.sum(jnp.where(hit, held, 0.0), axis=0, keepdims=True))
        return jnp.concatenate(rows, axis=0)

    def stat_copy(buf, mine, k, send, recv, peer):
        return pltpu.make_async_remote_copy(
            src_ref=buf.at[mine], dst_ref=buf.at[mine],
            send_sem=send.at[k], recv_sem=recv.at[mine],
            device_id=peer, device_id_type=MESH,
        )

    def spread(buf, mine, peers, send, recv, place_of):
        for k, p in enumerate(peers):
            stat_copy(buf, mine, k, send, recv, place_of(p)).start()

    def collect(buf, mine, peers, send, recv, place_of):
        total = buf[mine]
        for p in peers:
            stat_copy(buf, p, 0, send, recv, place_of(p)).wait_recv()
            total = total + buf[p]
        for k, p in enumerate(peers):
            stat_copy(buf, mine, k, send, recv, place_of(p)).wait_send()
        return total

    over_col = (stat_c, col, c_peers, sc_send, sc_recv, lambda p: (row, p))
    over_row = (stat_r, row, r_peers, sr_send, sr_recv, lambda p: (p, col))

    def one_level(level, carry):
        for h in range(halves - 1):
            take_x(level, h)
        take_z(level, halves - 1)

        @pl.when(level == LEVELS - 1)
        def _():
            rows = stat_rows(depth_t[...].T, held_t[...].T, range(1, LEVELS))
            stat_c[col, pl.ds(0, 2 * LEVELS - 2)] = rows
            stat_c[col, pl.ds(2 * LEVELS - 2, 2)] = jnp.zeros((2, rows.shape[1]), jnp.float32)
            spread(*over_col)

        for h in range(halves - 1):
            close(level, h)
        take_x(level, halves - 1)

        @pl.when(level < LEVELS - 1)
        def _():
            for h in range(halves - 1):
                take_z(level + 1, h)

        @pl.when(level == LEVELS - 1)
        def _():
            stat_r[row] = collect(*over_col)
            spread(*over_row)

        close(level, halves - 1)
        return carry

    for h in range(halves - 1):
        take_z(0, h)
    lax.fori_loop(0, LEVELS, one_level, 0)

    depth = depth_t[...].T
    held = held_t[...].T
    stat_f[me] = stat_rows(depth, held, [LEVELS])

    def final_copy(part_ref, peer):
        return pltpu.make_async_remote_copy(
            src_ref=part_ref, dst_ref=part_ref, send_sem=sf_sem.at[0], recv_sem=sf_sem.at[1],
            device_id=peer, device_id_type=MESH,
        )

    def tell(k, carry):
        final_copy(stat_f.at[me], device(k)).start()
        return carry

    lax.fori_loop(1, n_all, tell, 0)
    depth_out[...] = depth
    sums = collect(*over_row)
    others = final_copy(stat_f.at[pl.ds(0, n_all - 1)], device(1))
    others.wait_recv()
    others.wait_send()
    sums = jnp.concatenate([sums[:2 * LEVELS - 2], jnp.sum(stat_f[...], axis=0)], axis=0)

    scaling = jnp.ones((1, sums.shape[1]), jnp.float32)
    factor = jnp.zeros_like(held)
    for level in range(1, LEVELS + 1):
        count = sums[2 * level - 2:2 * level - 1]
        total = sums[2 * level - 1:2 * level]
        scaling = scaling / jnp.maximum(scaling * total / jnp.maximum(count, 1.0), 1.0)
        factor = jnp.where(depth == level, scaling, factor)
    reach_out[...] = frontier_ref[...].astype(jnp.float32) + factor * held


def search(frontier, visited, rows, cols, tiles, n_row, n_col):
    blocks, slots, tile, unused = tiles.shape
    per_dev, sources = frontier.shape
    places = (per_dev // tile) * (n_col * per_dev // tile)
    table = (blocks, 128 * (max(slots, places) // 128 + 1))
    n_core = 2 if n_col % 2 == 0 else 1
    n_x = n_col // n_core
    n_x = n_x if n_row % n_x == 0 else 1
    width = sources // HALVES
    dma = pltpu.SemaphoreType.DMA
    vmem = pl.BlockSpec(memory_space=pltpu.VMEM)
    return pl.pallas_call(
        functools.partial(search_kernel, n_row, n_col, n_x, n_core),
        out_shape=(
            jax.ShapeDtypeStruct((per_dev, sources), jnp.int32),
            jax.ShapeDtypeStruct((per_dev, sources), jnp.float32),
        ),
        in_specs=[vmem, vmem, vmem, vmem, pl.BlockSpec(memory_space=pl.ANY)],
        out_specs=(vmem, vmem),
        scratch_shapes=[
            pltpu.VMEM((blocks, slots + 1, tile, tile), jnp.bfloat16),
            pltpu.VMEM(table, jnp.int32),
            pltpu.VMEM(table, jnp.int32),
            pltpu.VMEM(table, jnp.int32),
            pltpu.SMEM(table, jnp.int32),
            pltpu.SMEM(table, jnp.int32),
            pltpu.VMEM((n_row, n_col, per_dev, per_dev), jnp.bfloat16),
            pltpu.VMEM((LEVELS + 1, HALVES, n_row, width, per_dev), jnp.bfloat16),
            pltpu.VMEM((HALVES, n_col, width, per_dev), jnp.float32),
            pltpu.VMEM((LEVELS, HALVES, n_col, width, per_dev), jnp.bfloat16),
            pltpu.VMEM((LEVELS, HALVES, n_col, width, per_dev), jnp.bfloat16),
            pltpu.VMEM((sources, per_dev), jnp.int32),
            pltpu.VMEM((sources, per_dev), jnp.float32),
            pltpu.VMEM((n_col, 2 * LEVELS, sources), jnp.float32),
            pltpu.VMEM((n_row, 2 * LEVELS, sources), jnp.float32),
            dma((n_row,)),
            dma((2,)),
            dma((2, HALVES, n_row)),
            dma((2, HALVES, n_row)),
            dma((2, HALVES, n_col)),
            dma((2, HALVES, n_col)),
            dma((n_col,)),
            dma((n_col,)),
            dma((n_row,)),
            dma((n_row,)),
            pltpu.VMEM((n_row * n_col, 2, sources), jnp.float32),
            dma((2,)),
        ],
        compiler_params=pltpu.CompilerParams(
            collective_id=0, has_side_effects=True, vmem_limit_bytes=60 * 1024 * 1024
        ),
        name="search",
    )(frontier, visited, rows, cols, tiles)


def solution(mesh):
    n_row, n_col = mesh.shape["row"], mesh.shape["col"]

    def on_device(frontier, visited, tile_rows, tile_cols, tile_bits):
        return search(
            frontier, visited, tile_rows[0, 0], tile_cols[0, 0], tile_bits[0, 0], n_row, n_col
        )

    placed = (
        P(("row", "col"), None),
        P(("row", "col"), None),
        P("row", "col", None, None),
        P("row", "col", None, None),
        P("row", "col", None, None, None, None),
    )
    return jax.shard_map(
        on_device,
        mesh=mesh,
        in_specs=placed,
        out_specs=(P(("row", "col"), None), P(("row", "col"), None)),
        check_vma=False,
    )
```
